32 devices in a mesh: lat: 4 (over x, core), lon: 8 (over z, y).
Axes of the slice: x: 2, y: 2, z: 4, core: 2. Of those that a mesh axis runs over, the one named last changes fastest.
Arguments:
- tokens: bfloat16 [4, 56, 32, 1536], P(None, 'lat', 'lon'), may hold values from -400 to 400, as said below
- in_bounds: int32 [5], replicated, may hold values from 0 to 47, as said below
- out_bounds: int32 [5], replicated, may hold values from 0 to 24, as said below
- down_gain: float32 [768], replicated, may hold values from 0.25 to 1.75
- down_bias: float32 [768], replicated, may hold values from -1 to 1
- down_weight: bfloat16 [768, 384], replicated, may hold values from -0.21875 to 0.21875
- up_weight: bfloat16 [384, 768], replicated, may hold values from -0.3125 to 0.3125
- up_gain: float32 [192], replicated, may hold values from 0.25 to 1.75
- up_bias: float32 [192], replicated, may hold values from -1 to 1
- out_weight: bfloat16 [192, 192], replicated, may hold values from -0.4375 to 0.4375
Outputs:
- merged: bfloat16 [4, 32, 16, 3072], P(None, 'lat', 'lon')
- upsampled: bfloat16 [4, 56, 32, 1536], P(None, 'lat', 'lon')
The draws below stay inside these ranges and needn't reach their ends.
Inputs may be any that keep to these rules, and one draw needn't show every extreme that they name: `tokens`: band b's fine rows stand in its slots from the first one on; slots past the band's count hold values that no output reads. in_bounds[0] = 0, in_bounds[4] = 47; each band has 10 to 14 fine rows, and some band has 14. out_bounds[0] = 0, out_bounds[4] = 24; each band has 4 to 8 merged rows, and some band has 8. For 0 < b < 4, 2 * out_bounds[b] - in_bounds[b] is 1 to 3, and 3 for some b; so merged band b covers fine rows from band b's first on to at most 3 rows past its last (fine row 47 counting as zeros), and band b's fine rows need merged rows from at most 2 rows before merged band b's first up to its last, 2 being reached.
All inputs are finite; a program needn't handle non-finite values.
Results may differ from the reference program's by a relative error of at most 0.0069.
Values may be sent and summed in bfloat16 or wider, within the bound.
A program may use at most 64 MiB of HBM per device.

```python
import math
import jax
import jax.numpy as jnp
from jax import lax

C = 192
LEV = 8
ROWS_DEV = 12
LON_DEV = 4
MEMBERS = 4
LCAP = 14
MCAP = 8
LAT = 47
MLAT = 24
LON = 32
N_LAT = 4
N_LON = 8


def pick_three(pattern, first, second, third):
    return jnp.where(pattern == 0, first, jnp.where(pattern == 1, second, third))


def bound_pair(key):
    base_key = jax.random.fold_in(key, 11)
    key_index, key_pattern, key_extra = jax.random.split(base_key, 3)
    places = jnp.arange(N_LAT + 1, dtype=jnp.int32)
    coarse_table = jnp.array([0, 1, 1, 1, 2], jnp.int32)
    fine_table = jnp.array([-1, -1, 0, 1, 1], jnp.int32)
    choose = jax.random.randint(key_index, (N_LAT + 1,), 0, 5).astype(jnp.int32)
    coarse_moves = jnp.take(coarse_table, choose)
    fine_moves = jnp.take(fine_table, choose)
    pattern = jax.random.randint(key_pattern, (), 0, 3).astype(jnp.int32)
    extra = jax.random.randint(key_extra, (), -1, 2).astype(jnp.int32)
    coarse_one = pick_three(pattern, 0, 2, coarse_moves[1])
    fine_one = pick_three(pattern, -1, 1, fine_moves[1])
    coarse_two = pick_three(pattern, 2, 0, 0)
    fine_two = pick_three(pattern, 1, -1, -1)
    coarse_three = pick_three(pattern, 1, jnp.where(extra > 0, 2, 1), 2)
    fine_three = pick_three(pattern, extra, 1, 1)
    coarse_moves = jnp.where(places == 1, coarse_one, jnp.where(places == 2, coarse_two, jnp.where(places == 3, coarse_three, coarse_moves)))
    fine_moves = jnp.where(places == 1, fine_one, jnp.where(places == 2, fine_two, jnp.where(places == 3, fine_three, fine_moves)))
    edges = (places == 0) | (places == N_LAT)
    fine_moves = jnp.where(edges, 0, fine_moves)
    coarse_moves = jnp.where(edges, 0, coarse_moves)
    fine_bounds = places * ROWS_DEV + fine_moves
    fine_bounds = jnp.where(places == N_LAT, N_LAT * ROWS_DEV - 1, fine_bounds)
    coarse_bounds = places * (ROWS_DEV // 2) + coarse_moves
    return (fine_bounds.astype(jnp.int32), coarse_bounds.astype(jnp.int32))


def draw_in_bounds(key, part):
    return bound_pair(key)[0]


def draw_out_bounds(key, part):
    return bound_pair(key)[1]


def draw_tokens(key, part):
    key_base, key_rows, key_chan = jax.random.split(jax.random.fold_in(key, 5), 3)
    shape = (MEMBERS, N_LAT * (ROWS_DEV + 2), LON_DEV * N_LON, LEV * C)
    row_scale = jnp.exp(jax.random.uniform(key_rows, (MEMBERS, N_LAT * (ROWS_DEV + 2), LON_DEV * N_LON, 1), jnp.float32, 0.0, math.log(10.0)))
    chan_scale = jnp.exp(jax.random.uniform(key_chan, (1, 1, 1, LEV * C), jnp.float32, 0.0, math.log(10.0)))
    values = jnp.clip(jax.random.normal(key_base, shape, jnp.float32), -4.0, 4.0)
    return (values * row_scale * chan_scale).astype(jnp.bfloat16)


def bell_draw(stream_key, shape, width, reach, kind=jnp.bfloat16):
    return jnp.clip(width * jax.random.normal(stream_key, shape, jnp.float32), -reach, reach).astype(kind)


def setup_inputs(seed: int = 0) -> dict:
    seeds = jax.random.split(jax.random.key(seed), 11)
    return {
        "tokens": draw_tokens(jax.random.fold_in(seeds[10], 71), 0),
        "in_bounds": draw_in_bounds(jax.random.fold_in(seeds[10], 71), 0),
        "out_bounds": draw_out_bounds(jax.random.fold_in(seeds[10], 71), 0),
        "down_gain": jnp.clip(1.0 + 0.15 * jax.random.normal(seeds[3], (4 * C,), jnp.float32), 0.25, 1.75),
        "down_bias": bell_draw(seeds[4], (4 * C,), 0.3, 1.0, jnp.float32),
        "down_weight": bell_draw(seeds[5], (4 * C, 2 * C), (4 * C) ** -0.5, 0.21875),
        "up_weight": bell_draw(seeds[6], (2 * C, 4 * C), (2 * C) ** -0.5, 0.3125),
        "up_gain": jnp.clip(1.0 + 0.15 * jax.random.normal(seeds[7], (C,), jnp.float32), 0.25, 1.75),
        "up_bias": bell_draw(seeds[8], (C,), 0.3, 1.0, jnp.float32),
        "out_weight": bell_draw(seeds[9], (C, C), C ** -0.5, 0.4375),
    }


def layer_norm(values, scale_vec, shift_vec):
    center = lax.optimization_barrier(jnp.mean(values, axis=-1, keepdims=True))
    spread = lax.optimization_barrier(jnp.mean(jnp.square(values - center), axis=-1, keepdims=True))
    return (values - center) * lax.rsqrt(spread + 1e-05) * scale_vec + shift_vec

def reference(tokens, in_bounds, out_bounds, down_gain, down_bias, down_weight, up_weight, up_gain, up_bias, out_weight):
    half_lon = LON // 2
    lat_rows = jnp.arange(LAT, dtype=jnp.int32)
    band_of = lax.optimization_barrier(jnp.sum((lat_rows[:, None] >= in_bounds[None, 1:N_LAT]).astype(jnp.int32), axis=1)).astype(jnp.int32)
    slot_of = (band_of * LCAP + lat_rows - in_bounds[band_of]).astype(jnp.int32)

    def one_member(member):
        token_grid = jnp.take(member, slot_of, axis=0)
        token_grid = jnp.concatenate([token_grid, jnp.zeros((1, LON, LEV * C), jnp.bfloat16)], axis=0)
        token_grid = jnp.roll(token_grid, 1, axis=1)
        pieces = token_grid.reshape(MLAT, 2, half_lon, 2, LEV, C).transpose(0, 2, 4, 3, 1, 5).reshape(-1, 4 * C)
        normed = layer_norm(pieces.astype(jnp.float32), down_gain, down_bias).astype(jnp.bfloat16)
        coarse = jnp.dot(normed, down_weight, preferred_element_type=jnp.float32).astype(jnp.bfloat16)
        widened = jnp.dot(coarse, up_weight, preferred_element_type=jnp.float32).astype(jnp.bfloat16)
        widened = widened.reshape(MLAT, half_lon, LEV, 2, 2, C).transpose(0, 4, 1, 3, 2, 5).reshape(2 * MLAT, LON, LEV, C)
        widened = jnp.roll(widened, -1, axis=1)[:LAT]
        renormed = layer_norm(widened.astype(jnp.float32), up_gain, up_bias).astype(jnp.bfloat16)
        finished = jnp.dot(renormed.reshape(-1, C), out_weight, preferred_element_type=jnp.float32).astype(jnp.bfloat16)
        return (coarse.reshape(MLAT, half_lon, LEV * 2 * C), finished.reshape(LAT, LON, LEV * C))
    coarse_all, fine_all = lax.map(one_member, tokens)
    fine_slots = jnp.arange(N_LAT * LCAP, dtype=jnp.int32)
    fine_band = (fine_slots // LCAP).astype(jnp.int32)
    fine_offset = (fine_slots % LCAP).astype(jnp.int32)
    fine_source = jnp.clip(in_bounds[fine_band] + fine_offset, 0, LAT - 1).astype(jnp.int32)
    fine_live = fine_offset < in_bounds[fine_band + 1] - in_bounds[fine_band]
    upsampled = jnp.where(fine_live[None, :, None, None], jnp.take(fine_all, fine_source, axis=1), jnp.zeros((), jnp.bfloat16))
    coarse_slots = jnp.arange(N_LAT * MCAP, dtype=jnp.int32)
    coarse_band = (coarse_slots // MCAP).astype(jnp.int32)
    coarse_offset = (coarse_slots % MCAP).astype(jnp.int32)
    coarse_source = jnp.clip(out_bounds[coarse_band] + coarse_offset, 0, MLAT - 1).astype(jnp.int32)
    coarse_live = coarse_offset < out_bounds[coarse_band + 1] - out_bounds[coarse_band]
    merged = jnp.where(coarse_live[None, :, None, None], jnp.take(coarse_all, coarse_source, axis=1), jnp.zeros((), jnp.bfloat16))
    return (merged.astype(jnp.bfloat16), upsampled.astype(jnp.bfloat16))
```

```python
import functools

import jax
import jax.numpy as jnp
from jax import lax
from jax.experimental import pallas as pl
from jax.experimental.pallas import tpu as pltpu
from jax.sharding import PartitionSpec as P

HALO = 3
LANES_OF_LEVELS = 4
MESH = pl.DeviceIdType.MESH


def norm(values, scale_vec, shift_vec):
    center = jnp.mean(values, axis=-1, keepdims=True)
    off = values - center
    spread = jnp.mean(off * off, axis=-1, keepdims=True)
    return off * lax.rsqrt(spread + 1e-05) * scale_vec + shift_vec


def kernel(
    n_lat,
    n_lon,
    in_b,
    out_b,
    t_ref,
    dw_hbm,
    uw_hbm,
    ow_hbm,
    dg_ref,
    db_ref,
    ug_ref,
    ub_ref,
    mo_ref,
    fo_ref,
    comb,
    west_in,
    east_in,
    top_in,
    bot_in,
    top_w,
    top_e,
    bot_w,
    bot_e,
    tail,
    tail_w,
    tail_e,
    nrm,
    dw,
    uw,
    ow,
    local_sem,
    send_sem,
    recv_sem,
):
    cols, slots, sub, lanes = t_ref.shape
    chan = lanes // LANES_OF_LEVELS
    total = slots + 2 * HALO
    rows = 2 * mo_ref.shape[0] + 4
    mid_lo, mid_hi = HALO, slots // 2
    lat = lax.axis_index("lat")
    lon = lax.axis_index("lon")
    east = {"lat": lat, "lon": lax.rem(lon + 1, n_lon)}
    west = {"lat": lat, "lon": lax.rem(lon + n_lon - 1, n_lon)}
    above = {"lat": jnp.maximum(lat - 1, 0), "lon": lon}
    below = {"lat": jnp.minimum(lat + 1, n_lat - 1), "lon": lon}
    has_above = lat > 0
    has_below = lat < n_lat - 1

    loads = [
        pltpu.make_async_copy(t_ref, comb.at[pl.ds(1, cols), pl.ds(HALO, slots)], local_sem.at[0]),
        pltpu.make_async_copy(dw_hbm, dw, local_sem.at[1]),
        pltpu.make_async_copy(uw_hbm, uw, local_sem.at[2]),
        pltpu.make_async_copy(ow_hbm, ow, local_sem.at[3]),
    ]
    for load in loads:
        load.start()

    barrier = pltpu.get_barrier_semaphore()
    pl.semaphore_signal(barrier, inc=1, device_id=east, device_id_type=MESH)
    pl.semaphore_signal(barrier, inc=1, device_id=west, device_id_type=MESH)

    @pl.when(has_above)
    def _():
        pl.semaphore_signal(barrier, inc=1, device_id=above, device_id_type=MESH)

    @pl.when(has_below)
    def _():
        pl.semaphore_signal(barrier, inc=1, device_id=below, device_id_type=MESH)

    pl.semaphore_wait(barrier, 2 + has_above.astype(jnp.int32) + has_below.astype(jnp.int32))

    def remote(src, dst, slot, device):
        return pltpu.make_async_remote_copy(
            src_ref=src,
            dst_ref=dst,
            send_sem=send_sem.at[slot],
            recv_sem=recv_sem.at[slot],
            device_id=device,
            device_id_type=MESH,
        )

    spans = [(0, mid_lo), (mid_hi, slots), (mid_lo, mid_hi)]
    to_east, to_west = [], []
    for i, (lo, hi) in enumerate(spans):
        span = pl.ds(lo, hi - lo)
        to_east.append(remote(t_ref.at[cols - 1, span], west_in.at[span], i, east))
        to_west.append(remote(t_ref.at[0, span], east_in.at[span], 3 + i, west))
    up = remote(t_ref.at[:, pl.ds(0, HALO)], bot_in, 6, above)
    down = remote(tail, top_in, 7, below)
    head = pl.ds(0, HALO)
    up_w = remote(west_in.at[head], bot_w, 8, above)
    up_e = remote(east_in.at[head], bot_e, 9, above)
    down_w = remote(tail_w, top_w, 10, below)
    down_e = remote(tail_e, top_e, 11, below)

    for i in range(2):
        to_east[i].start()
        to_west[i].start()

    @pl.when(has_above)
    def _():
        up.start()

    to_east[2].start()
    to_west[2].start()

    start_in = in_b[lat]
    end_in = in_b[lat + 1]
    count = end_in - start_in
    shift = 2 * out_b[lat] - start_in
    past = count - shift + 4

    loads[0].wait()
    for x in range(cols):
        for i in range(HALO):
            tail[x, i] = comb[1 + x, count + i]

    @pl.when(has_below)
    def _():
        down.start()

    for load in loads[1:]:
        load.wait()

    def place(r):
        inside = jnp.maximum(r + shift - 1, 0)
        outside = jnp.minimum(HALO + slots + r - past, total - 1)
        return jnp.where(r < past, inside, outside)

    spots = [place(r) for r in range(rows)]

    dg = dg_ref[...]
    db = db_ref[...]
    ug = ug_ref[...]
    ub = ub_ref[...]

    def compute(j, ms):
        nm = len(ms)
        size = LANES_OF_LEVELS * nm * sub
        for k in range(0, nm, 2):
            blocks = []
            for c in range(2):
                for a in range(2):
                    blocks.append(
                        jnp.concatenate(
                            [comb[2 * j + c, spots[2 * m + a]].astype(jnp.float32) for m in ms[k : k + 2]],
                            axis=0,
                        )
                    )
            for level in range(LANES_OF_LEVELS):
                cut = slice(level * chan, (level + 1) * chan)
                pieces = jnp.concatenate([block[:, cut] for block in blocks], axis=1)
                at = (level * nm + k) * sub
                nrm[at : at + 2 * sub, :] = norm(pieces, dg, db).astype(jnp.bfloat16)
        wide = jnp.dot(nrm[0:size, :], dw[...], preferred_element_type=jnp.float32)
        coarse = wide.astype(jnp.bfloat16)
        if j < 2:
            for i, m in enumerate(ms):
                if m < 2:
                    continue
                for level in range(LANES_OF_LEVELS):
                    at = (level * nm + i) * sub
                    mo_ref[m - 2, j, :, level * 2 * chan : (level + 1) * 2 * chan] = wide[
                        at : at + sub
                    ].astype(jnp.bfloat16)
        for c, x in (((1, 0),), ((0, 1), (1, 2)), ((0, 3),))[j]:
            spread = jnp.dot(
                coarse, uw[:, c * 2 * chan : (c + 1) * 2 * chan], preferred_element_type=jnp.float32
            ).astype(jnp.bfloat16)
            spread = spread.astype(jnp.float32)
            for a in range(2):
                half = norm(spread[:, a * chan : (a + 1) * chan], ug, ub).astype(jnp.bfloat16)
                done = jnp.dot(half, ow[...], preferred_element_type=jnp.float32)
                for i, m in enumerate(ms):
                    fo_ref[2 * m + a, x] = jnp.concatenate(
                        [
                            done[(level * nm + i) * sub : (level * nm + i + 1) * sub]
                            for level in range(LANES_OF_LEVELS)
                        ],
                        axis=1,
                    ).astype(jnp.bfloat16)

    own = pl.ds(1, cols)

    @pl.when(has_above)
    def _():
        down.wait_recv()

    @pl.when(has_below)
    def _():
        up.wait_recv()
        comb[own, HALO + slots : total] = bot_in[...]

    @pl.when(jnp.logical_not(has_below))
    def _():
        comb[:, HALO + slots : total] = jnp.zeros((cols + 2, HALO, sub, lanes), jnp.bfloat16)

    @pl.when(has_above)
    def _():
        comb[own, 0:HALO] = top_in[...]

    @pl.when(jnp.logical_not(has_above))
    def _():
        comb[:, 0:HALO] = jnp.zeros((cols + 2, HALO, sub, lanes), jnp.bfloat16)

    merged_rows = rows // 2
    compute(1, list(range(merged_rows)))

    for i in range(2):
        lo, hi = spans[i]
        to_east[i].wait_recv()
        comb[0, HALO + lo : HALO + hi] = west_in[lo:hi]
        to_west[i].wait_recv()
        comb[cols + 1, HALO + lo : HALO + hi] = east_in[lo:hi]
    for i in range(HALO):
        tail_w[i] = comb[0, count + i]
        tail_e[i] = comb[cols + 1, count + i]

    @pl.when(has_above)
    def _():
        up_w.start()
        up_e.start()

    @pl.when(has_below)
    def _():
        down_w.start()
        down_e.start()

    lo, hi = spans[2]
    to_east[2].wait_recv()
    comb[0, HALO + lo : HALO + hi] = west_in[lo:hi]
    to_west[2].wait_recv()
    comb[cols + 1, HALO + lo : HALO + hi] = east_in[lo:hi]

    @pl.when(has_above)
    def _():
        down_w.wait_recv()
        comb[0, 0:HALO] = top_w[...]
        down_e.wait_recv()
        comb[cols + 1, 0:HALO] = top_e[...]

    @pl.when(has_below)
    def _():
        up_w.wait_recv()
        comb[0, HALO + slots : total] = bot_w[...]
        up_e.wait_recv()
        comb[cols + 1, HALO + slots : total] = bot_e[...]

    compute(0, list(range(merged_rows)))
    compute(2, list(range(merged_rows)))

    for copy in to_east + to_west:
        copy.wait_send()

    @pl.when(has_above)
    def _():
        up.wait_send()
        up_w.wait_send()
        up_e.wait_send()

    @pl.when(has_below)
    def _():
        down.wait_send()
        down_w.wait_send()
        down_e.wait_send()


def body(
    tokens,
    in_bounds,
    out_bounds,
    down_gain,
    down_bias,
    down_weight,
    up_weight,
    up_gain,
    up_bias,
    out_weight,
):
    members, slots, cols, packed = tokens.shape
    chan = down_weight.shape[0] // 4
    halves = packed // (chan * LANES_OF_LEVELS)
    lanes = chan * LANES_OF_LEVELS
    sub = halves * members
    merged_slots = slots // 2 + 1
    half_cols = cols // 2
    rows = 2 * merged_slots + 4
    total = slots + 2 * HALO
    bf16 = jnp.bfloat16
    n_lat = lax.axis_size("lat")
    n_lon = lax.axis_size("lon")
    grid_tokens = tokens.reshape(members, slots, cols, halves, lanes)
    grid_tokens = grid_tokens.transpose(2, 1, 3, 0, 4).reshape(cols, slots, sub, lanes)
    smem = pl.BlockSpec(memory_space=pltpu.SMEM)
    vmem = pl.BlockSpec(memory_space=pltpu.VMEM)
    hbm = pl.BlockSpec(memory_space=pl.ANY)
    column = pltpu.VMEM((slots, sub, lanes), bf16)
    patch = pltpu.VMEM((cols, HALO, sub, lanes), bf16)
    corner = pltpu.VMEM((HALO, sub, lanes), bf16)
    merged_raw, fine_raw = pl.pallas_call(
        functools.partial(kernel, n_lat, n_lon),
        out_shape=(
            jax.ShapeDtypeStruct((merged_slots, half_cols, sub, 2 * lanes), bf16),
            jax.ShapeDtypeStruct((rows, cols, sub, lanes), bf16),
        ),
        in_specs=[smem, smem, hbm, hbm, hbm, hbm, vmem, vmem, vmem, vmem],
        out_specs=(vmem, vmem),
        scratch_shapes=[
            pltpu.VMEM((cols + 2, total, sub, lanes), bf16),
            column,
            column,
            patch,
            patch,
            corner,
            corner,
            corner,
            corner,
            patch,
            corner,
            corner,
            pltpu.VMEM((LANES_OF_LEVELS * rows // 2 * sub, 4 * chan), bf16),
            pltpu.VMEM(down_weight.shape, bf16),
            pltpu.VMEM(up_weight.shape, bf16),
            pltpu.VMEM(out_weight.shape, bf16),
            pltpu.SemaphoreType.DMA((4,)),
            pltpu.SemaphoreType.DMA((12,)),
            pltpu.SemaphoreType.DMA((12,)),
        ],
        compiler_params=pltpu.CompilerParams(collective_id=0, has_side_effects=True),
    )(
        in_bounds,
        out_bounds,
        grid_tokens,
        down_weight,
        up_weight,
        out_weight,
        down_gain[None],
        down_bias[None],
        up_gain[None],
        up_bias[None],
    )
    band = lax.axis_index("lat")
    count_in = in_bounds[band + 1] - in_bounds[band]
    count_out = out_bounds[band + 1] - out_bounds[band]
    shift = 2 * out_bounds[band] - in_bounds[band]
    zero = jnp.zeros((), bf16)
    merged = merged_raw.reshape(merged_slots, half_cols, halves, members, 2 * lanes)
    merged = merged.transpose(3, 0, 1, 2, 4).reshape(members, merged_slots, half_cols, 2 * packed)
    merged_live = jnp.arange(merged_slots, dtype=jnp.int32) < count_out
    merged = jnp.where(merged_live[None, :, None, None], merged, zero)
    fine = lax.dynamic_slice_in_dim(fine_raw, 4 - shift, slots, 0)
    fine = fine.reshape(slots, cols, halves, members, lanes).transpose(3, 0, 1, 2, 4)
    fine = fine.reshape(members, slots, cols, packed)
    fine_live = jnp.arange(slots, dtype=jnp.int32) < count_in
    return merged, jnp.where(fine_live[None, :, None, None], fine, zero)


def solution(mesh):
    return jax.shard_map(
        body,
        mesh=mesh,
        in_specs=(P(None, "lat", "lon", None), P(), P(), P(), P(), P(), P(), P(), P(), P()),
        out_specs=(P(None, "lat", "lon", None), P(None, "lat", "lon", None)),
        check_vma=False,
    )
```

```python
import functools

import jax
import jax.numpy as jnp
from jax import lax
from jax.experimental import pallas as pl
from jax.experimental.pallas import tpu as pltpu
from jax.sharding import PartitionSpec as P

HALO = 3
LANES_OF_LEVELS = 4
TILE = 128
MESH = pl.DeviceIdType.MESH


def norm(values, scale_vec, shift_vec):
    center = jnp.mean(values, axis=-1, keepdims=True)
    off = values - center
    spread = jnp.mean(off * off, axis=-1, keepdims=True)
    return off * lax.rsqrt(spread + 1e-05) * scale_vec + shift_vec


def kernel(
    n_lat,
    n_lon,
    in_b,
    out_b,
    t_ref,
    dw_hbm,
    uw_hbm,
    ow_hbm,
    dg_ref,
    db_ref,
    ug_ref,
    ub_ref,
    mo_ref,
    fo_ref,
    comb,
    west_in,
    east_in,
    top_in,
    bot_in,
    top_w,
    top_e,
    bot_w,
    bot_e,
    tail,
    tail_w,
    tail_e,
    nrm,
    turn_in,
    turn_merged,
    turn_fine,
    dw,
    uw,
    ow,
    local_sem,
    send_sem,
    recv_sem,
):
    members, slots, cols, packed = t_ref.shape
    merged_slots = mo_ref.shape[1]
    _, _, sub, lanes = comb.shape
    halves = sub // members
    chan = lanes // LANES_OF_LEVELS
    tiles = lanes // TILE
    total = slots + 2 * HALO
    rows = 2 * merged_slots + 4
    mid_lo, mid_hi = HALO, slots // 2
    lat = lax.axis_index("lat")
    lon = lax.axis_index("lon")
    east = {"lat": lat, "lon": lax.rem(lon + 1, n_lon)}
    west = {"lat": lat, "lon": lax.rem(lon + n_lon - 1, n_lon)}
    above = {"lat": jnp.maximum(lat - 1, 0), "lon": lon}
    below = {"lat": jnp.minimum(lat + 1, n_lat - 1), "lon": lon}
    has_above = lat > 0
    has_below = lat < n_lat - 1

    loads = [
        pltpu.make_async_copy(dw_hbm, dw, local_sem.at[0]),
        pltpu.make_async_copy(uw_hbm, uw, local_sem.at[1]),
        pltpu.make_async_copy(ow_hbm, ow, local_sem.at[2]),
    ]
    for load in loads:
        load.start()

    barrier = pltpu.get_barrier_semaphore()
    pl.semaphore_signal(barrier, inc=1, device_id=east, device_id_type=MESH)
    pl.semaphore_signal(barrier, inc=1, device_id=west, device_id_type=MESH)

    @pl.when(has_above)
    def _():
        pl.semaphore_signal(barrier, inc=1, device_id=above, device_id_type=MESH)

    @pl.when(has_below)
    def _():
        pl.semaphore_signal(barrier, inc=1, device_id=below, device_id_type=MESH)

    for r in range(slots):
        for member in range(members):
            row = t_ref[member, r].astype(jnp.float32)
            for half in range(halves):
                at = (half * members + member) * cols
                for t in range(tiles):
                    lane = half * lanes + t * TILE
                    turn_in[r, t, at : at + cols, :] = row[:, lane : lane + TILE]

    def take_column(x):
        for r in range(slots):
            for t in range(tiles):
                comb[1 + x, HALO + r, :, t * TILE : (t + 1) * TILE] = turn_in[
                    r, t, pl.ds(x, sub, stride=cols), :
                ].astype(jnp.bfloat16)

    take_column(cols - 1)
    take_column(0)

    pl.semaphore_wait(barrier, 2 + has_above.astype(jnp.int32) + has_below.astype(jnp.int32))

    def remote(src, dst, slot, device):
        return pltpu.make_async_remote_copy(
            src_ref=src,
            dst_ref=dst,
            send_sem=send_sem.at[slot],
            recv_sem=recv_sem.at[slot],
            device_id=device,
            device_id_type=MESH,
        )

    spans = [(0, mid_lo), (mid_hi, slots), (mid_lo, mid_hi)]
    to_east, to_west = [], []
    for i, (lo, hi) in enumerate(spans):
        span = pl.ds(lo, hi - lo)
        held = pl.ds(HALO + lo, hi - lo)
        to_east.append(remote(comb.at[cols, held], west_in.at[span], i, east))
        to_west.append(remote(comb.at[1, held], east_in.at[span], 3 + i, west))
    up = remote(comb.at[pl.ds(1, cols), pl.ds(HALO, HALO)], bot_in, 6, above)
    down = remote(tail, top_in, 7, below)
    head = pl.ds(0, HALO)
    up_w = remote(west_in.at[head], bot_w, 8, above)
    up_e = remote(east_in.at[head], bot_e, 9, above)
    down_w = remote(tail_w, top_w, 10, below)
    down_e = remote(tail_e, top_e, 11, below)

    for i in range(3):
        to_east[i].start()
        to_west[i].start()

    for x in range(1, cols - 1):
        take_column(x)

    @pl.when(has_above)
    def _():
        up.start()

    start_in = in_b[lat]
    end_in = in_b[lat + 1]
    count = end_in - start_in
    shift = 2 * out_b[lat] - start_in
    past = count - shift + 4

    for x in range(cols):
        for i in range(HALO):
            tail[x, i] = comb[1 + x, count + i]

    @pl.when(has_below)
    def _():
        down.start()

    for load in loads:
        load.wait()

    def place(r):
        inside = jnp.maximum(r + shift - 1, 0)
        outside = jnp.minimum(HALO + slots + r - past, total - 1)
        return jnp.where(r < past, inside, outside)

    spots = [place(r) for r in range(rows)]

    dg = dg_ref[...][None]
    db = db_ref[...][None]
    ug = ug_ref[...][None]
    ub = ub_ref[...][None]

    def compute(j, ms):
        nm = len(ms)
        size = LANES_OF_LEVELS * nm * sub
        for k in range(0, nm, 2):
            blocks = []
            for c in range(2):
                for a in range(2):
                    blocks.append(
                        jnp.concatenate(
                            [comb[2 * j + c, spots[2 * m + a]].astype(jnp.float32) for m in ms[k : k + 2]],
                            axis=0,
                        )
                    )
            for level in range(LANES_OF_LEVELS):
                cut = slice(level * chan, (level + 1) * chan)
                pieces = jnp.concatenate([block[:, cut] for block in blocks], axis=1)
                at = (level * nm + k) * sub
                nrm[at : at + 2 * sub, :] = norm(pieces, dg, db).astype(jnp.bfloat16)
        wide = jnp.dot(nrm[0:size, :], dw[...], preferred_element_type=jnp.float32)
        coarse = wide.astype(jnp.bfloat16)
        if j < 2:
            for i, m in enumerate(ms):
                if m < 2:
                    continue
                for level in range(LANES_OF_LEVELS):
                    at = (level * nm + i) * sub
                    for t in range(2 * chan // TILE):
                        turn_merged[
                            m - 2, level * 2 * chan // TILE + t, pl.ds(j, sub, stride=cols // 2), :
                        ] = wide[at : at + sub, t * TILE : (t + 1) * TILE]
        for c, x in (((1, 0),), ((0, 1), (1, 2)), ((0, 3),))[j]:
            spread = jnp.dot(
                coarse, uw[:, c * 2 * chan : (c + 1) * 2 * chan], preferred_element_type=jnp.float32
            ).astype(jnp.bfloat16)
            spread = spread.astype(jnp.float32)
            for a in range(2):
                half = norm(spread[:, a * chan : (a + 1) * chan], ug, ub).astype(jnp.bfloat16)
                done = jnp.dot(half, ow[...], preferred_element_type=jnp.float32)
                for i, m in enumerate(ms):
                    line = jnp.concatenate(
                        [
                            done[(level * nm + i) * sub : (level * nm + i + 1) * sub]
                            for level in range(LANES_OF_LEVELS)
                        ],
                        axis=1,
                    )
                    for t in range(tiles):
                        turn_fine[2 * m + a, t, pl.ds(x, sub, stride=cols), :] = line[
                            :, t * TILE : (t + 1) * TILE
                        ]

    own = pl.ds(1, cols)

    @pl.when(has_above)
    def _():
        down.wait_recv()

    @pl.when(has_below)
    def _():
        up.wait_recv()
        comb[own, HALO + slots : total] = bot_in[...]

    @pl.when(jnp.logical_not(has_below))
    def _():
        comb[:, HALO + slots : total] = jnp.zeros((cols + 2, HALO, sub, lanes), jnp.bfloat16)

    @pl.when(has_above)
    def _():
        comb[own, 0:HALO] = top_in[...]

    @pl.when(jnp.logical_not(has_above))
    def _():
        comb[:, 0:HALO] = jnp.zeros((cols + 2, HALO, sub, lanes), jnp.bfloat16)

    merged_rows = rows // 2
    compute(1, list(range(merged_rows)))

    for i in range(2):
        lo, hi = spans[i]
        to_east[i].wait_recv()
        comb[0, HALO + lo : HALO + hi] = west_in[lo:hi]
        to_west[i].wait_recv()
        comb[cols + 1, HALO + lo : HALO + hi] = east_in[lo:hi]
    for i in range(HALO):
        tail_w[i] = comb[0, count + i]
        tail_e[i] = comb[cols + 1, count + i]

    @pl.when(has_above)
    def _():
        up_w.start()
        up_e.start()

    @pl.when(has_below)
    def _():
        down_w.start()
        down_e.start()

    lo, hi = spans[2]
    to_east[2].wait_recv()
    comb[0, HALO + lo : HALO + hi] = west_in[lo:hi]
    to_west[2].wait_recv()
    comb[cols + 1, HALO + lo : HALO + hi] = east_in[lo:hi]

    @pl.when(has_above)
    def _():
        down_w.wait_recv()
        comb[0, 0:HALO] = top_w[...]
        down_e.wait_recv()
        comb[cols + 1, 0:HALO] = top_e[...]

    @pl.when(has_below)
    def _():
        up_w.wait_recv()
        comb[0, HALO + slots : total] = bot_w[...]
        up_e.wait_recv()
        comb[cols + 1, HALO + slots : total] = bot_e[...]

    def put_out(value, live, slot, out_ref, width, span):
        value = jnp.where(live, value, 0.0).astype(jnp.bfloat16)
        for half in range(halves):
            for member in range(members):
                at = (half * members + member) * width
                out_ref[member, slot, :, half * span : (half + 1) * span] = jnp.concatenate(
                    [value[t, at : at + width] for t in range(span // TILE)], axis=1
                )

    compute(0, list(range(merged_rows)))
    count_out = out_b[lat + 1] - out_b[lat]
    for m in range(merged_slots):
        put_out(turn_merged[m], m < count_out, m, mo_ref, cols // 2, 2 * lanes)
    compute(2, list(range(merged_rows)))
    for k in range(slots):
        put_out(turn_fine[4 - shift + k], k < count, k, fo_ref, cols, lanes)

    for copy in to_east + to_west:
        copy.wait_send()

    @pl.when(has_above)
    def _():
        up.wait_send()
        up_w.wait_send()
        up_e.wait_send()

    @pl.when(has_below)
    def _():
        down.wait_send()
        down_w.wait_send()
        down_e.wait_send()


def body(
    tokens,
    in_bounds,
    out_bounds,
    down_gain,
    down_bias,
    down_weight,
    up_weight,
    up_gain,
    up_bias,
    out_weight,
):
    members, slots, cols, packed = tokens.shape
    chan = down_weight.shape[0] // 4
    halves = packed // (chan * LANES_OF_LEVELS)
    lanes = chan * LANES_OF_LEVELS
    sub = halves * members
    merged_slots = slots // 2 + 1
    half_cols = cols // 2
    rows = 2 * merged_slots + 4
    total = slots + 2 * HALO
    bf16 = jnp.bfloat16
    n_lat = lax.axis_size("lat")
    n_lon = lax.axis_size("lon")
    smem = pl.BlockSpec(memory_space=pltpu.SMEM)
    vmem = pl.BlockSpec(memory_space=pltpu.VMEM)
    hbm = pl.BlockSpec(memory_space=pl.ANY)
    column = pltpu.VMEM((slots, sub, lanes), bf16)
    patch = pltpu.VMEM((cols, HALO, sub, lanes), bf16)
    corner = pltpu.VMEM((HALO, sub, lanes), bf16)
    return pl.pallas_call(
        functools.partial(kernel, n_lat, n_lon),
        out_shape=(
            jax.ShapeDtypeStruct((members, merged_slots, half_cols, 2 * packed), bf16),
            jax.ShapeDtypeStruct(tokens.shape, bf16),
        ),
        in_specs=[smem, smem, vmem, hbm, hbm, hbm, vmem, vmem, vmem, vmem],
        out_specs=(vmem, vmem),
        scratch_shapes=[
            pltpu.VMEM((cols + 2, total, sub, lanes), bf16),
            column,
            column,
            patch,
            patch,
            corner,
            corner,
            corner,
            corner,
            patch,
            corner,
            corner,
            pltpu.VMEM((LANES_OF_LEVELS * rows // 2 * sub, 4 * chan), bf16),
            pltpu.VMEM((slots, lanes // TILE, sub * cols, TILE), jnp.float32),
            pltpu.VMEM((merged_slots, 2 * lanes // TILE, sub * half_cols, TILE), jnp.float32),
            pltpu.VMEM((rows, lanes // TILE, sub * cols, TILE), jnp.float32),
            pltpu.VMEM(down_weight.shape, bf16),
            pltpu.VMEM(up_weight.shape, bf16),
            pltpu.VMEM(out_weight.shape, bf16),
            pltpu.SemaphoreType.DMA((3,)),
            pltpu.SemaphoreType.DMA((12,)),
            pltpu.SemaphoreType.DMA((12,)),
        ],
        compiler_params=pltpu.CompilerParams(collective_id=0, has_side_effects=True),
    )(
        in_bounds,
        out_bounds,
        tokens,
        down_weight,
        up_weight,
        out_weight,
        down_gain,
        down_bias,
        up_gain,
        up_bias,
    )


def solution(mesh):
    return jax.shard_map(
        body,
        mesh=mesh,
        in_specs=(P(None, "lat", "lon", None), P(), P(), P(), P(), P(), P(), P(), P(), P()),
        out_specs=(P(None, "lat", "lon", None), P(None, "lat", "lon", None)),
        check_vma=False,
    )
```

```python
import functools

import jax
import jax.numpy as jnp
from jax import lax
from jax.experimental import pallas as pl
from jax.experimental.pallas import tpu as pltpu
from jax.sharding import PartitionSpec as P

HALO = 3
LANES_OF_LEVELS = 4
TILE = 128
MESH = pl.DeviceIdType.MESH


def norm(values, scale_vec, shift_vec):
    center = jnp.mean(values, axis=-1, keepdims=True)
    off = values - center
    spread = jnp.mean(off * off, axis=-1, keepdims=True)
    return off * lax.rsqrt(spread + 1e-05) * scale_vec + shift_vec


def kernel(
    n_lat,
    n_lon,
    in_b,
    out_b,
    t_ref,
    dw_hbm,
    uw_hbm,
    ow_hbm,
    dg_ref,
    db_ref,
    ug_ref,
    ub_ref,
    mo_ref,
    fo_ref,
    comb,
    side_in,
    top_in,
    bot_in,
    top_c,
    bot_c,
    tail,
    tail_c,
    nrm,
    turn_in,
    turn_merged,
    turn_fine,
    dw,
    uw,
    ow,
    local_sem,
    send_sem,
    recv_sem,
):
    members, slots, cols, packed = t_ref.shape
    merged_slots = mo_ref.shape[1]
    _, _, sub, lanes = comb.shape
    halves = sub // members
    chan = lanes // LANES_OF_LEVELS
    tiles = lanes // TILE
    total = slots + 2 * HALO
    rows = 2 * merged_slots + 4
    mid_lo, mid_hi = HALO, slots // 2
    lat = lax.axis_index("lat")
    lon = lax.axis_index("lon")
    odd = lax.rem(lon, 2)
    far = {"lat": lat, "lon": lax.rem(lon + n_lon - 1 + 2 * odd, n_lon)}
    near = {"lat": lat, "lon": lax.rem(lon + 1 + (n_lon - 2) * odd, n_lon)}
    above = {"lat": jnp.maximum(lat - 1, 0), "lon": lon}
    below = {"lat": jnp.minimum(lat + 1, n_lat - 1), "lon": lon}
    has_above = lat > 0
    has_below = lat < n_lat - 1

    loads = [
        pltpu.make_async_copy(dw_hbm, dw, local_sem.at[0]),
        pltpu.make_async_copy(uw_hbm.at[:, pl.ds(0, 2 * chan)], uw.at[0], local_sem.at[1]),
        pltpu.make_async_copy(uw_hbm.at[:, pl.ds(2 * chan, 2 * chan)], uw.at[1], local_sem.at[2]),
        pltpu.make_async_copy(ow_hbm, ow, local_sem.at[3]),
    ]
    for load in loads:
        load.start()

    barrier = pltpu.get_barrier_semaphore()
    pl.semaphore_signal(barrier, inc=1, device_id=far, device_id_type=MESH)
    pl.semaphore_signal(barrier, inc=1, device_id=near, device_id_type=MESH)

    @pl.when(has_above)
    def _():
        pl.semaphore_signal(barrier, inc=1, device_id=above, device_id_type=MESH)

    @pl.when(has_below)
    def _():
        pl.semaphore_signal(barrier, inc=1, device_id=below, device_id_type=MESH)

    for r in range(slots):
        for member in range(members):
            row = t_ref[member, r].astype(jnp.float32)
            for half in range(halves):
                at = (half * members + member) * cols
                for t in range(tiles):
                    lane = half * lanes + t * TILE
                    turn_in[r, t, at : at + cols, :] = row[:, lane : lane + TILE]

    def take_column(x):
        for r in range(slots):
            for t in range(tiles):
                comb[1 + x, HALO + r, :, t * TILE : (t + 1) * TILE] = turn_in[
                    r, t, pl.ds(x, sub, stride=cols), :
                ].astype(jnp.bfloat16)

    take_column(cols - 1)
    take_column(0)

    pl.semaphore_wait(barrier, 2 + has_above.astype(jnp.int32) + has_below.astype(jnp.int32))

    def remote(src, dst, slot, device):
        return pltpu.make_async_remote_copy(
            src_ref=src,
            dst_ref=dst,
            send_sem=send_sem.at[slot],
            recv_sem=recv_sem.at[slot],
            device_id=device,
            device_id_type=MESH,
        )

    sides = (odd, 1 - odd)
    spans = [(0, mid_lo), (mid_hi, slots), (mid_lo, mid_hi)]
    far_copy = remote(
        comb.at[1 + odd * (cols - 1), pl.ds(HALO, slots)], side_in.at[1 - odd], 0, far
    )
    near_copies = [
        remote(
            comb.at[cols - odd * (cols - 1), pl.ds(HALO + lo, hi - lo)],
            side_in.at[odd, pl.ds(lo, hi - lo)],
            1 + i,
            near,
        )
        for i, (lo, hi) in enumerate(spans)
    ]
    up = remote(comb.at[pl.ds(1, cols), pl.ds(HALO, HALO)], bot_in, 4, above)
    down = remote(tail, top_in, 5, below)
    up_c = [remote(side_in.at[sides[o], pl.ds(0, HALO)], bot_c.at[o], 6 + o, above) for o in range(2)]
    down_c = [remote(tail_c.at[o], top_c.at[o], 8 + o, below) for o in range(2)]

    far_copy.start()
    for copy in near_copies:
        copy.start()

    for x in range(1, cols - 1):
        take_column(x)

    @pl.when(has_above)
    def _():
        up.start()

    start_in = in_b[lat]
    end_in = in_b[lat + 1]
    count = end_in - start_in
    shift = 2 * out_b[lat] - start_in
    past = count - shift + 4

    for x in range(cols):
        for i in range(HALO):
            tail[x, i] = comb[1 + x, count + i]

    @pl.when(has_below)
    def _():
        down.start()

    for load in loads:
        load.wait()

    def place(r):
        inside = jnp.maximum(r + shift - 1, 0)
        outside = jnp.minimum(HALO + slots + r - past, total - 1)
        return jnp.where(r < past, inside, outside)

    spots = [place(r) for r in range(rows)]

    dg = dg_ref[...][None]
    db = db_ref[...][None]
    ug = ug_ref[...][None]
    ub = ub_ref[...][None]

    def compute(base, ms, targets, merged_at):
        nm = len(ms)
        size = LANES_OF_LEVELS * nm * sub
        for k in range(0, nm, 2):
            blocks = []
            for c in range(2):
                for a in range(2):
                    blocks.append(
                        jnp.concatenate(
                            [comb[base + c, spots[2 * m + a]].astype(jnp.float32) for m in ms[k : k + 2]],
                            axis=0,
                        )
                    )
            for level in range(LANES_OF_LEVELS):
                cut = slice(level * chan, (level + 1) * chan)
                pieces = jnp.concatenate([block[:, cut] for block in blocks], axis=1)
                at = (level * nm + k) * sub
                nrm[at : at + 2 * sub, :] = norm(pieces, dg, db).astype(jnp.bfloat16)
        wide = jnp.dot(nrm[0:size, :], dw[...], preferred_element_type=jnp.float32)
        coarse = wide.astype(jnp.bfloat16)
        if merged_at is not None:
            merged_half, j = merged_at
            for i, m in enumerate(ms):
                if m < 2:
                    continue
                for level in range(LANES_OF_LEVELS):
                    at = (level * nm + i) * sub
                    for t in range(2 * chan // TILE):
                        turn_merged[
                            merged_half * merged_slots + m - 2, level * 2 * chan // TILE + t, pl.ds(j, sub, stride=cols // 2), :
                        ] = wide[at : at + sub, t * TILE : (t + 1) * TILE]
        for c, x in targets:
            spread = jnp.dot(
                coarse, uw[c], preferred_element_type=jnp.float32
            ).astype(jnp.bfloat16)
            spread = spread.astype(jnp.float32)
            for a in range(2):
                half = norm(spread[:, a * chan : (a + 1) * chan], ug, ub).astype(jnp.bfloat16)
                done = jnp.dot(half, ow[...], preferred_element_type=jnp.float32)
                for i, m in enumerate(ms):
                    line = jnp.concatenate(
                        [
                            done[(level * nm + i) * sub : (level * nm + i + 1) * sub]
                            for level in range(LANES_OF_LEVELS)
                        ],
                        axis=1,
                    )
                    for t in range(tiles):
                        turn_fine[2 * m + a, t, pl.ds(x, sub, stride=cols), :] = line[
                            :, t * TILE : (t + 1) * TILE
                        ]

    own = pl.ds(1, cols)

    @pl.when(has_above)
    def _():
        down.wait_recv()

    @pl.when(has_below)
    def _():
        up.wait_recv()
        comb[own, HALO + slots : total] = bot_in[...]

    @pl.when(jnp.logical_not(has_below))
    def _():
        comb[:, HALO + slots : total] = jnp.zeros((cols + 2, HALO, sub, lanes), jnp.bfloat16)

    @pl.when(has_above)
    def _():
        comb[own, 0:HALO] = top_in[...]

    @pl.when(jnp.logical_not(has_above))
    def _():
        comb[:, 0:HALO] = jnp.zeros((cols + 2, HALO, sub, lanes), jnp.bfloat16)

    merged_rows = rows // 2
    compute(2, list(range(merged_rows)), ((0, 1), (1, 2)), (0, 1))

    def compute_side(o, ms):
        side = sides[o]
        compute(side * cols, ms, ((1 - side, side * (cols - 1)),), (side, 0))

    def arrive(o, lo, hi):
        comb[sides[o] * (cols + 1), HALO + lo : HALO + hi] = side_in[sides[o], lo:hi]

    def pass_corners(o):
        for i in range(HALO):
            tail_c[o, i] = comb[sides[o] * (cols + 1), count + i]

        @pl.when(has_above)
        def _():
            up_c[o].start()

        @pl.when(has_below)
        def _():
            down_c[o].start()

    def take_corners(o):
        @pl.when(has_above)
        def _():
            down_c[o].wait_recv()
            comb[sides[o] * (cols + 1), 0:HALO] = top_c[o]

        @pl.when(has_below)
        def _():
            up_c[o].wait_recv()
            comb[sides[o] * (cols + 1), HALO + slots : total] = bot_c[o]

    inner = [2, 3]
    outer = [m for m in range(merged_rows) if m not in inner]
    far_copy.wait_recv()
    arrive(0, 0, slots)
    pass_corners(0)
    compute_side(0, inner)
    take_corners(0)
    for i in range(2):
        near_copies[i].wait_recv()
        arrive(1, *spans[i])
    pass_corners(1)
    compute_side(0, outer)
    near_copies[2].wait_recv()
    arrive(1, *spans[2])
    take_corners(1)
    compute_side(1, list(range(merged_rows)))

    def put_out(value, live, slot, out_ref, width, span):
        value = jnp.where(live, value, 0.0).astype(jnp.bfloat16)
        for half in range(halves):
            for member in range(members):
                at = (half * members + member) * width
                out_ref[member, slot, :, half * span : (half + 1) * span] = jnp.concatenate(
                    [value[t, at : at + width] for t in range(span // TILE)], axis=1
                )

    count_out = out_b[lat + 1] - out_b[lat]
    for m in range(merged_slots):
        put_out(turn_merged[m], m < count_out, m, mo_ref, cols // 2, 2 * lanes)
    for k in range(slots):
        put_out(turn_fine[4 - shift + k], k < count, k, fo_ref, cols, lanes)

    far_copy.wait_send()
    for copy in near_copies:
        copy.wait_send()

    @pl.when(has_above)
    def _():
        up.wait_send()
        for copy in up_c:
            copy.wait_send()

    @pl.when(has_below)
    def _():
        down.wait_send()
        for copy in down_c:
            copy.wait_send()


def body(
    tokens,
    in_bounds,
    out_bounds,
    down_gain,
    down_bias,
    down_weight,
    up_weight,
    up_gain,
    up_bias,
    out_weight,
):
    members, slots, cols, packed = tokens.shape
    chan = down_weight.shape[0] // 4
    halves = packed // (chan * LANES_OF_LEVELS)
    lanes = chan * LANES_OF_LEVELS
    sub = halves * members
    merged_slots = slots // 2 + 1
    half_cols = cols // 2
    rows = 2 * merged_slots + 4
    total = slots + 2 * HALO
    bf16 = jnp.bfloat16
    n_lat = lax.axis_size("lat")
    n_lon = lax.axis_size("lon")
    smem = pl.BlockSpec(memory_space=pltpu.SMEM)
    vmem = pl.BlockSpec(memory_space=pltpu.VMEM)
    hbm = pl.BlockSpec(memory_space=pl.ANY)
    patch = pltpu.VMEM((cols, HALO, sub, lanes), bf16)
    corners = pltpu.VMEM((2, HALO, sub, lanes), bf16)
    return pl.pallas_call(
        functools.partial(kernel, n_lat, n_lon),
        out_shape=(
            jax.ShapeDtypeStruct((members, merged_slots, half_cols, 2 * packed), bf16),
            jax.ShapeDtypeStruct(tokens.shape, bf16),
        ),
        in_specs=[smem, smem, vmem, hbm, hbm, hbm, vmem, vmem, vmem, vmem],
        out_specs=(vmem, vmem),
        scratch_shapes=[
            pltpu.VMEM((cols + 2, total, sub, lanes), bf16),
            pltpu.VMEM((2, slots, sub, lanes), bf16),
            patch,
            patch,
            corners,
            corners,
            patch,
            corners,
            pltpu.VMEM((LANES_OF_LEVELS * rows // 2 * sub, 4 * chan), bf16),
            pltpu.VMEM((slots, lanes // TILE, sub * cols, TILE), jnp.float32),
            pltpu.VMEM((2 * merged_slots, 2 * lanes // TILE, sub * half_cols, TILE), jnp.float32),
            pltpu.VMEM((rows, lanes // TILE, sub * cols, TILE), jnp.float32),
            pltpu.VMEM(down_weight.shape, bf16),
            pltpu.VMEM((2, 2 * chan, 2 * chan), bf16),
            pltpu.VMEM(out_weight.shape, bf16),
            pltpu.SemaphoreType.DMA((4,)),
            pltpu.SemaphoreType.DMA((10,)),
            pltpu.SemaphoreType.DMA((10,)),
        ],
        compiler_params=pltpu.CompilerParams(collective_id=0, has_side_effects=True),
    )(
        in_bounds,
        out_bounds,
        tokens,
        down_weight,
        up_weight,
        out_weight,
        down_gain,
        down_bias,
        up_gain,
        up_bias,
    )


def solution(mesh):
    return jax.shard_map(
        body,
        mesh=mesh,
        in_specs=(P(None, "lat", "lon", None), P(), P(), P(), P(), P(), P(), P(), P(), P()),
        out_specs=(P(None, "lat", "lon", None), P(None, "lat", "lon", None)),
        check_vma=False,
    )
```

```python
import functools

import jax
import jax.numpy as jnp
from jax import lax
from jax.experimental import pallas as pl
from jax.experimental.pallas import tpu as pltpu
from jax.sharding import PartitionSpec as P

HALO = 3
LANES_OF_LEVELS = 4
TILE = 128
MESH = pl.DeviceIdType.MESH


def norm(values, scale_vec, shift_vec):
    center = jnp.mean(values, axis=-1, keepdims=True)
    off = values - center
    spread = jnp.mean(off * off, axis=-1, keepdims=True)
    return off * lax.rsqrt(spread + 1e-05) * scale_vec + shift_vec


def kernel(
    n_lat,
    n_lon,
    in_b,
    out_b,
    t_ref,
    dw_hbm,
    uw_hbm,
    ow_hbm,
    dg_ref,
    db_ref,
    ug_ref,
    ub_ref,
    mo_ref,
    fo_ref,
    comb,
    west_in,
    east_in,
    top_in,
    bot_in,
    top_w,
    top_e,
    bot_w,
    bot_e,
    tail,
    tail_w,
    tail_e,
    nrm,
    turn_in,
    turn_merged,
    turn_fine,
    dw,
    uw,
    ow,
    local_sem,
    send_sem,
    recv_sem,
):
    members, slots, cols, packed = t_ref.shape
    merged_slots = mo_ref.shape[1]
    _, _, sub, lanes = comb.shape
    halves = sub // members
    chan = lanes // LANES_OF_LEVELS
    tiles = lanes // TILE
    total = slots + 2 * HALO
    rows = 2 * merged_slots + 4
    mid_lo, mid_hi = HALO, slots // 2
    lat = lax.axis_index("lat")
    lon = lax.axis_index("lon")
    east = {"lat": lat, "lon": lax.rem(lon + 1, n_lon)}
    west = {"lat": lat, "lon": lax.rem(lon + n_lon - 1, n_lon)}
    above = {"lat": jnp.maximum(lat - 1, 0), "lon": lon}
    below = {"lat": jnp.minimum(lat + 1, n_lat - 1), "lon": lon}
    has_above = lat > 0
    has_below = lat < n_lat - 1

    loads = [
        pltpu.make_async_copy(dw_hbm, dw, local_sem.at[0]),
        pltpu.make_async_copy(uw_hbm, uw, local_sem.at[1]),
        pltpu.make_async_copy(ow_hbm, ow, local_sem.at[2]),
    ]
    for load in loads:
        load.start()

    barrier = pltpu.get_barrier_semaphore()
    pl.semaphore_signal(barrier, inc=1, device_id=east, device_id_type=MESH)
    pl.semaphore_signal(barrier, inc=1, device_id=west, device_id_type=MESH)

    @pl.when(has_above)
    def _():
        pl.semaphore_signal(barrier, inc=1, device_id=above, device_id_type=MESH)

    @pl.when(has_below)
    def _():
        pl.semaphore_signal(barrier, inc=1, device_id=below, device_id_type=MESH)

    for r in range(slots):
        for member in range(members):
            row = t_ref[member, r].astype(jnp.float32)
            for half in range(halves):
                at = (half * members + member) * cols
                for t in range(tiles):
                    lane = half * lanes + t * TILE
                    turn_in[r, t, at : at + cols, :] = row[:, lane : lane + TILE]

    def take_column(x):
        for r in range(slots):
            for t in range(tiles):
                comb[1 + x, HALO + r, :, t * TILE : (t + 1) * TILE] = turn_in[
                    r, t, pl.ds(x, sub, stride=cols), :
                ].astype(jnp.bfloat16)

    take_column(cols - 1)
    take_column(0)

    pl.semaphore_wait(barrier, 2 + has_above.astype(jnp.int32) + has_below.astype(jnp.int32))

    def remote(src, dst, slot, device):
        return pltpu.make_async_remote_copy(
            src_ref=src,
            dst_ref=dst,
            send_sem=send_sem.at[slot],
            recv_sem=recv_sem.at[slot],
            device_id=device,
            device_id_type=MESH,
        )

    spans = [(0, mid_lo), (mid_hi, slots), (mid_lo, mid_hi)]
    to_east, to_west = [], []
    for i, (lo, hi) in enumerate(spans):
        span = pl.ds(lo, hi - lo)
        held = pl.ds(HALO + lo, hi - lo)
        to_east.append(remote(comb.at[cols, held], west_in.at[span], i, east))
        to_west.append(remote(comb.at[1, held], east_in.at[span], 3 + i, west))
    up = remote(comb.at[pl.ds(1, cols), pl.ds(HALO, HALO)], bot_in, 6, above)
    down = remote(tail, top_in, 7, below)
    head = pl.ds(0, HALO)
    up_w = remote(west_in.at[head], bot_w, 8, above)
    up_e = remote(east_in.at[head], bot_e, 9, above)
    down_w = remote(tail_w, top_w, 10, below)
    down_e = remote(tail_e, top_e, 11, below)

    for i in range(3):
        to_east[i].start()
        to_west[i].start()

    for x in range(1, cols - 1):
        take_column(x)

    @pl.when(has_above)
    def _():
        up.start()

    start_in = in_b[lat]
    end_in = in_b[lat + 1]
    count = end_in - start_in
    shift = 2 * out_b[lat] - start_in
    past = count - shift + 4

    for x in range(cols):
        for i in range(HALO):
            tail[x, i] = comb[1 + x, count + i]

    @pl.when(has_below)
    def _():
        down.start()

    for load in loads:
        load.wait()

    def place(r):
        inside = jnp.maximum(r + shift - 1, 0)
        outside = jnp.minimum(HALO + slots + r - past, total - 1)
        return jnp.where(r < past, inside, outside)

    spots = [place(r) for r in range(rows)]

    dg = dg_ref[...][None]
    db = db_ref[...][None]
    ug = ug_ref[...][None]
    ub = ub_ref[...][None]

    def compute(j, ms):
        nm = len(ms)
        size = LANES_OF_LEVELS * nm * sub
        for k in range(0, nm, 2):
            blocks = []
            for c in range(2):
                for a in range(2):
                    blocks.append(
                        jnp.concatenate(
                            [comb[2 * j + c, spots[2 * m + a]].astype(jnp.float32) for m in ms[k : k + 2]],
                            axis=0,
                        )
                    )
            for level in range(LANES_OF_LEVELS):
                cut = slice(level * chan, (level + 1) * chan)
                pieces = jnp.concatenate([block[:, cut] for block in blocks], axis=1)
                at = (level * nm + k) * sub
                nrm[at : at + 2 * sub, :] = norm(pieces, dg, db).astype(jnp.bfloat16)
        wide = jnp.dot(nrm[0:size, :], dw[...], preferred_element_type=jnp.float32)
        coarse = wide.astype(jnp.bfloat16)
        if j < 2:
            for i, m in enumerate(ms):
                if m < 2:
                    continue
                for level in range(LANES_OF_LEVELS):
                    at = (level * nm + i) * sub
                    for t in range(2 * chan // TILE):
                        turn_merged[
                            m - 2, level * 2 * chan // TILE + t, pl.ds(j, sub, stride=cols // 2), :
                        ] = wide[at : at + sub, t * TILE : (t + 1) * TILE]
        for c, x in (((1, 0),), ((0, 1), (1, 2)), ((0, 3),))[j]:
            spread = jnp.dot(
                coarse, uw[:, c * 2 * chan : (c + 1) * 2 * chan], preferred_element_type=jnp.float32
            ).astype(jnp.bfloat16)
            spread = spread.astype(jnp.float32)
            for a in range(2):
                half = norm(spread[:, a * chan : (a + 1) * chan], ug, ub).astype(jnp.bfloat16)
                done = jnp.dot(half, ow[...], preferred_element_type=jnp.float32)
                for i, m in enumerate(ms):
                    line = jnp.concatenate(
                        [
                            done[(level * nm + i) * sub : (level * nm + i + 1) * sub]
                            for level in range(LANES_OF_LEVELS)
                        ],
                        axis=1,
                    )
                    for t in range(tiles):
                        turn_fine[2 * m + a, t, pl.ds(x, sub, stride=cols), :] = line[
                            :, t * TILE : (t + 1) * TILE
                        ]

    own = pl.ds(1, cols)

    @pl.when(has_above)
    def _():
        down.wait_recv()

    @pl.when(has_below)
    def _():
        up.wait_recv()
        comb[own, HALO + slots : total] = bot_in[...]

    @pl.when(jnp.logical_not(has_below))
    def _():
        comb[:, HALO + slots : total] = jnp.zeros((cols + 2, HALO, sub, lanes), jnp.bfloat16)

    @pl.when(has_above)
    def _():
        comb[own, 0:HALO] = top_in[...]

    @pl.when(jnp.logical_not(has_above))
    def _():
        comb[:, 0:HALO] = jnp.zeros((cols + 2, HALO, sub, lanes), jnp.bfloat16)

    merged_rows = rows // 2
    compute(1, list(range(merged_rows)))

    for i in range(2):
        lo, hi = spans[i]
        to_east[i].wait_recv()
        comb[0, HALO + lo : HALO + hi] = west_in[lo:hi]
        to_west[i].wait_recv()
        comb[cols + 1, HALO + lo : HALO + hi] = east_in[lo:hi]
    for i in range(HALO):
        tail_w[i] = comb[0, count + i]
        tail_e[i] = comb[cols + 1, count + i]

    @pl.when(has_above)
    def _():
        up_w.start()
        up_e.start()

    @pl.when(has_below)
    def _():
        down_w.start()
        down_e.start()

    lo, hi = spans[2]
    to_east[2].wait_recv()
    comb[0, HALO + lo : HALO + hi] = west_in[lo:hi]
    to_west[2].wait_recv()
    comb[cols + 1, HALO + lo : HALO + hi] = east_in[lo:hi]

    @pl.when(has_above)
    def _():
        down_w.wait_recv()
        comb[0, 0:HALO] = top_w[...]
        down_e.wait_recv()
        comb[cols + 1, 0:HALO] = top_e[...]

    @pl.when(has_below)
    def _():
        up_w.wait_recv()
        comb[0, HALO + slots : total] = bot_w[...]
        up_e.wait_recv()
        comb[cols + 1, HALO + slots : total] = bot_e[...]

    def put_out(value, live, slot, out_ref, width, span):
        value = jnp.where(live, value, 0.0).astype(jnp.bfloat16)
        for half in range(halves):
            for member in range(members):
                at = (half * members + member) * width
                out_ref[member, slot, :, half * span : (half + 1) * span] = jnp.concatenate(
                    [value[t, at : at + width] for t in range(span // TILE)], axis=1
                )

    compute(0, list(range(merged_rows)))
    count_out = out_b[lat + 1] - out_b[lat]
    for m in range(merged_slots):
        put_out(turn_merged[m], m < count_out, m, mo_ref, cols // 2, 2 * lanes)
    compute(2, list(range(merged_rows)))
    for k in range(slots):
        put_out(turn_fine[4 - shift + k], k < count, k, fo_ref, cols, lanes)

    for copy in to_east + to_west:
        copy.wait_send()

    @pl.when(has_above)
    def _():
        up.wait_send()
        up_w.wait_send()
        up_e.wait_send()

    @pl.when(has_below)
    def _():
        down.wait_send()
        down_w.wait_send()
        down_e.wait_send()


def body(
    tokens,
    in_bounds,
    out_bounds,
    down_gain,
    down_bias,
    down_weight,
    up_weight,
    up_gain,
    up_bias,
    out_weight,
):
    members, slots, cols, packed = tokens.shape
    chan = down_weight.shape[0] // 4
    halves = packed // (chan * LANES_OF_LEVELS)
    lanes = chan * LANES_OF_LEVELS
    sub = halves * members
    merged_slots = slots // 2 + 1
    half_cols = cols // 2
    rows = 2 * merged_slots + 4
    total = slots + 2 * HALO
    bf16 = jnp.bfloat16
    n_lat = lax.axis_size("lat")
    n_lon = lax.axis_size("lon")
    smem = pl.BlockSpec(memory_space=pltpu.SMEM)
    vmem = pl.BlockSpec(memory_space=pltpu.VMEM)
    hbm = pl.BlockSpec(memory_space=pl.ANY)
    column = pltpu.VMEM((slots, sub, lanes), bf16)
    patch = pltpu.VMEM((cols, HALO, sub, lanes), bf16)
    corner = pltpu.VMEM((HALO, sub, lanes), bf16)
    return pl.pallas_call(
        functools.partial(kernel, n_lat, n_lon),
        out_shape=(
            jax.ShapeDtypeStruct((members, merged_slots, half_cols, 2 * packed), bf16),
            jax.ShapeDtypeStruct(tokens.shape, bf16),
        ),
        in_specs=[smem, smem, vmem, hbm, hbm, hbm, vmem, vmem, vmem, vmem],
        out_specs=(vmem, vmem),
        scratch_shapes=[
            pltpu.VMEM((cols + 2, total, sub, lanes), bf16),
            column,
            column,
            patch,
            patch,
            corner,
            corner,
            corner,
            corner,
            patch,
            corner,
            corner,
            pltpu.VMEM((LANES_OF_LEVELS * rows // 2 * sub, 4 * chan), bf16),
            pltpu.VMEM((slots, lanes // TILE, sub * cols, TILE), jnp.float32),
            pltpu.VMEM((merged_slots, 2 * lanes // TILE, sub * half_cols, TILE), jnp.float32),
            pltpu.VMEM((rows, lanes // TILE, sub * cols, TILE), jnp.float32),
            pltpu.VMEM(down_weight.shape, bf16),
            pltpu.VMEM(up_weight.shape, bf16),
            pltpu.VMEM(out_weight.shape, bf16),
            pltpu.SemaphoreType.DMA((3,)),
            pltpu.SemaphoreType.DMA((12,)),
            pltpu.SemaphoreType.DMA((12,)),
        ],
        compiler_params=pltpu.CompilerParams(
            collective_id=0, has_side_effects=True, vmem_limit_bytes=24 * 1024 * 1024
        ),
    )(
        in_bounds,
        out_bounds,
        tokens,
        down_weight,
        up_weight,
        out_weight,
        down_gain,
        down_bias,
        up_gain,
        up_bias,
    )


def solution(mesh):
    return jax.shard_map(
        body,
        mesh=mesh,
        in_specs=(P(None, "lat", "lon", None), P(), P(), P(), P(), P(), P(), P(), P(), P()),
        out_specs=(P(None, "lat", "lon", None), P(None, "lat", "lon", None)),
        check_vma=False,
    )
```
